32 devices in a mesh: ctx: 16 (over z, y, x), head: 2 (over core).
Axes of the slice: x: 2, y: 2, z: 4, core: 2. Of those that a mesh axis runs over, the one named last changes fastest.
Arguments:
- probe_matrix: bfloat16 [8192, 4096], P('ctx', 'head'), may hold values from -6 to 6
- lookup_matrix: bfloat16 [8192, 4096], P('ctx', 'head'), may hold values from -6 to 6
- content_matrix: bfloat16 [8192, 4096], P('ctx', 'head'), may hold values from -6 to 6
- log_retention: float32 [32, 8192], P('head', 'ctx'), may hold values from -1.5 to 0
- following_observation_vector: bfloat16 [8192, 4096], P('ctx', 'head'), may hold values from -6 to 6
- rescaler_coefficients: float32 [4096], P('head'), may hold values from 0.25 to 1.75
- payoff_objective_coefficient: float32 [8192], P('ctx'), may hold values from 0.1 to 4
Outputs:
- surprise_payoff: float32 [8192], P('ctx')
- grad_queries: bfloat16 [8192, 4096], P('ctx', 'head')
- grad_keys: bfloat16 [8192, 4096], P('ctx', 'head')
- grad_values: bfloat16 [8192, 4096], P('ctx', 'head')
- scaling_derivative_mean: float32 [4096], P('head')
The draws below stay inside these ranges and needn't reach their ends.
All inputs are finite; a program needn't handle non-finite values.
Results may differ from the reference program's by a relative error of at most 0.0095.
Values may be sent and summed in bfloat16 or wider, within the bound.
A program may use at most 128 MiB of HBM per device.

```python
import math
import jax
import jax.numpy as jnp
from jax import lax

ATTENTION_HEADS = 32
HEAD_DIM = 128
TOK_DEV = 512
HIDDEN_DIMENSION = 4096
EPISODE_STEPS = 8192


def draw_log_retention(key, part):
    lookup_matrix = jax.random.split(jax.random.fold_in(key, 11), 6)
    slow_share = 0.5
    slow = jax.random.uniform(lookup_matrix[0], (ATTENTION_HEADS,), jnp.float32) < slow_share
    fast_rate = jnp.exp(jax.random.uniform(lookup_matrix[1], (ATTENTION_HEADS,), jnp.float32, math.log(1.0 / 50.0), math.log(1.0 / 30.0)))
    slow_rate = 0.6 / EPISODE_STEPS
    decay_rate = jnp.where(slow, slow_rate, fast_rate)
    blocks = EPISODE_STEPS // TOK_DEV
    block_multiplier = jnp.exp(jax.random.uniform(lookup_matrix[2], (ATTENTION_HEADS, blocks), jnp.float32, math.log(0.5), math.log(2.0)))
    block_multiplier = jnp.repeat(block_multiplier, TOK_DEV, axis=1)
    coarse_estimate = jax.random.uniform(lookup_matrix[3], (ATTENTION_HEADS, EPISODE_STEPS), jnp.float32, 0.5, 1.5)
    group_location = jax.random.randint(lookup_matrix[4], (ATTENTION_HEADS, 3), 0, EPISODE_STEPS)
    group_size = jnp.log(jax.random.uniform(lookup_matrix[5], (ATTENTION_HEADS, 3), jnp.float32, 0.5, 0.8))
    token_position = jnp.arange(EPISODE_STEPS, dtype=jnp.int32)
    token_groups = jnp.sum(jnp.where(token_position[None, None, :] == group_location[:, :, None], group_size[:, :, None], 0.0), axis=1)
    return -decay_rate[:, None] * block_multiplier * coarse_estimate + token_groups


def draw_payoff_objective_coefficient(key, part):
    lookup_matrix = jax.random.split(jax.random.fold_in(key, 23), 2)
    token_position = jnp.arange(EPISODE_STEPS, dtype=jnp.float32)
    ramp = 0.5 + 1.5 * token_position / (EPISODE_STEPS - 1)
    coarse_estimate = jax.random.uniform(lookup_matrix[1], (EPISODE_STEPS,), jnp.float32, 0.5, 1.5)
    return ramp * coarse_estimate


def level_of(own_key, shape, cuts, low, largest):
    def one(dim, blocks):
        heights = jax.random.uniform(jax.random.fold_in(jax.random.fold_in(own_key, 6), dim), (blocks,), jnp.float32, low / len(cuts), largest / len(cuts))
        return jnp.repeat(jnp.exp(heights), shape[dim] // blocks).reshape((-1,) + (1,) * (len(shape) - dim - 1))

    factor_of = one(*cuts[0])
    for cut in cuts[1:]:
        factor_of = factor_of * one(*cut)
    return factor_of


def normal_values(key, extent, deviation, most, shards=(), kind=jnp.bfloat16):
    values = jax.random.normal(key, extent, jnp.float32) * deviation
    if len(shards) > 0:
        values = level_of(key, extent, shards, -0.22, 0.18) * values
    return jnp.clip(values, min=-most, max=most).astype(kind)


def setup_inputs(seed: int = 0) -> dict:
    streams_of = jax.random.split(jax.random.key(seed), 8)
    return {
        "probe_matrix": normal_values(streams_of[0], (EPISODE_STEPS, HIDDEN_DIMENSION), 1.0, 6.0, ((0, 16), (1, 2))),
        "lookup_matrix": normal_values(streams_of[1], (EPISODE_STEPS, HIDDEN_DIMENSION), 1.0, 6.0, ((0, 16), (1, 2))),
        "content_matrix": normal_values(streams_of[2], (EPISODE_STEPS, HIDDEN_DIMENSION), 1.0, 6.0, ((0, 16), (1, 2))),
        "log_retention": draw_log_retention(jax.random.fold_in(streams_of[7], 71), 0),
        "following_observation_vector": normal_values(streams_of[4], (EPISODE_STEPS, HIDDEN_DIMENSION), 1.0, 6.0, ((0, 16), (1, 2))),
        "rescaler_coefficients": jnp.clip(1.0 + 0.15 * jax.random.normal(streams_of[5], (HIDDEN_DIMENSION,), jnp.float32), 0.25, 1.75),
        "payoff_objective_coefficient": draw_payoff_objective_coefficient(jax.random.fold_in(streams_of[7], 71), 0),
    }


EPS = 1e-06

def product(form, left, right):
    return jnp.einsum(form, left.astype(jnp.float32), right.astype(jnp.float32))

def block_parts(query_block, key_block, forget_block):
    cumulative = jnp.cumsum(forget_block, axis=1)
    count = forget_block.shape[1]
    token_position = jnp.arange(count, dtype=jnp.int32)
    causal = (token_position[:, None] >= token_position[None, :])[None]
    gaps = cumulative[:, :, None] - cumulative[:, None, :]
    decays = jnp.where(causal, jnp.exp(jnp.where(causal, gaps, jnp.float32(0.0))), jnp.float32(0.0))
    attn_scale = HEAD_DIM ** (-0.5)
    probs = (product('thd,shd->hts', query_block, key_block) * attn_scale * decays).astype(jnp.bfloat16)
    start_decay = jnp.exp(cumulative).T
    total = cumulative[:, -1]
    tail_decay = jnp.exp(total[:, None] - cumulative).T
    return (decays, probs, start_decay, total, tail_decay)

def forward_step(state, inputs):
    query_block, key_block, value_block, forget_block = inputs
    decays, probs, start_decay, total, tail_decay = block_parts(query_block, key_block, forget_block)
    attn_scale = HEAD_DIM ** (-0.5)
    local_part = product('hts,shd->thd', probs, value_block)
    state_low = state.astype(jnp.bfloat16)
    carried = product('thd,hde->the', query_block, state_low)
    attn_out = local_part + attn_scale * start_decay[:, :, None] * carried
    key_decayed = (key_block.astype(jnp.float32) * tail_decay[:, :, None]).astype(jnp.bfloat16)
    summary = product('shd,she->hde', key_decayed, value_block)
    new_state = jnp.exp(total)[:, None, None] * state + summary
    return (new_state, (attn_out, state_low))

def backward_step(state, inputs):
    query_block, key_block, value_block, forget_block, state_low, grad_out = inputs
    decays, probs, start_decay, total, tail_decay = block_parts(query_block, key_block, forget_block)
    attn_scale = HEAD_DIM ** (-0.5)
    later_low = state.astype(jnp.bfloat16)
    grad_probs = (product('the,she->hts', grad_out, value_block) * attn_scale * decays).astype(jnp.bfloat16)
    probe_derivative = product('hts,shd->thd', grad_probs, key_block) + attn_scale * start_decay[:, :, None] * product('the,hde->thd', grad_out, state_low)
    lookup_derivative = product('hts,thd->shd', grad_probs, query_block) + tail_decay[:, :, None] * product('she,hde->shd', value_block, later_low)
    content_derivative = product('hts,the->she', probs, grad_out) + tail_decay[:, :, None] * product('shd,hde->she', key_block, later_low)
    query_decayed = (query_block.astype(jnp.float32) * (attn_scale * start_decay)[:, :, None]).astype(jnp.bfloat16)
    back_summary = product('thd,the->hde', query_decayed, grad_out)
    new_state = back_summary + jnp.exp(total)[:, None, None] * state
    return (new_state, (probe_derivative.astype(jnp.bfloat16), lookup_derivative.astype(jnp.bfloat16), content_derivative.astype(jnp.bfloat16)))

def reference(probe_matrix, lookup_matrix, content_matrix, log_retention, following_observation_vector, rescaler_coefficients, payoff_objective_coefficient):
    blocks = EPISODE_STEPS // TOK_DEV

    def split(array):
        return array.reshape(blocks, TOK_DEV, ATTENTION_HEADS, HEAD_DIM)
    forget_blocks = log_retention.reshape(ATTENTION_HEADS, blocks, TOK_DEV).transpose(1, 0, 2)
    initial = jnp.zeros((ATTENTION_HEADS, HEAD_DIM, HEAD_DIM), jnp.float32)
    final_state, outputs = lax.scan(forward_step, initial, (split(probe_matrix), split(lookup_matrix), split(content_matrix), forget_blocks))
    attn_out, states = outputs
    output_flat = attn_out.reshape(EPISODE_STEPS, HIDDEN_DIMENSION)
    rms = jnp.sqrt(lax.optimization_barrier(jnp.sum(output_flat * output_flat, axis=1)) / HIDDEN_DIMENSION + EPS)
    rescaled_activations = output_flat / rms[:, None]
    predicted_minus_actual = rescaler_coefficients[None, :] * rescaled_activations - following_observation_vector.astype(jnp.float32)
    surprise_payoff = lax.optimization_barrier(jnp.sum(predicted_minus_actual * predicted_minus_actual, axis=1)) / HIDDEN_DIMENSION
    discrepancy_adjoint = payoff_objective_coefficient[:, None] * predicted_minus_actual
    normalized_adjoint = discrepancy_adjoint * rescaler_coefficients[None, :]
    inner_accumulation = lax.optimization_barrier(jnp.sum(normalized_adjoint * rescaled_activations, axis=1))
    grad_out = ((normalized_adjoint - rescaled_activations * (inner_accumulation / HIDDEN_DIMENSION)[:, None]) / rms[:, None]).astype(jnp.bfloat16)
    scaling_derivative_mean = lax.optimization_barrier(jnp.sum(discrepancy_adjoint * rescaled_activations, axis=0)) / EPISODE_STEPS
    first_state, grads = lax.scan(backward_step, initial, (split(probe_matrix), split(lookup_matrix), split(content_matrix), forget_blocks, states, split(grad_out)), reverse=True)
    probe_derivative, lookup_derivative, content_derivative = grads
    return (surprise_payoff, probe_derivative.reshape(EPISODE_STEPS, HIDDEN_DIMENSION), lookup_derivative.reshape(EPISODE_STEPS, HIDDEN_DIMENSION), content_derivative.reshape(EPISODE_STEPS, HIDDEN_DIMENSION), scaling_derivative_mean)
```

```python
import functools

import jax
import jax.numpy as jnp
from jax import lax
from jax.experimental import pallas as pl
from jax.experimental.pallas import tpu as pltpu
from jax.sharding import PartitionSpec as P

HEAD_DIM = 128
HIDDEN_DIMENSION = 4096
SCALE = HEAD_DIM ** (-0.5)
EPS = 1e-06
F32 = jnp.float32
BF16 = jnp.bfloat16


def mm(a, b, ca, cb):
    return lax.dot_general(a, b, (((ca,), (cb,)), ((), ())), preferred_element_type=F32)


def column(row):
    return jnp.broadcast_to(row, (HEAD_DIM, row.shape[1])).T


def decay_block(col, row, diagonal):
    gap = col[:, :1] - row
    dec = jnp.exp(gap)
    if diagonal:
        t = lax.broadcasted_iota(jnp.int32, gap.shape, 0)
        s = lax.broadcasted_iota(jnp.int32, gap.shape, 1)
        dec = jnp.where(t >= s, dec, 0.0)
    return dec * SCALE


def block_rows(tokens):
    return 256 if tokens % 256 == 0 else tokens


def summary_kernel(heads, k_ref, v_ref, cum_ref, out_ref):
    for h in range(heads):
        cols = slice(h * HEAD_DIM, (h + 1) * HEAD_DIM)
        row = cum_ref[h]
        tail = column(jnp.exp(row[:, -1:] - row))
        kd = (k_ref[:, cols].astype(F32) * tail).astype(BF16)
        out_ref[h] = mm(kd, v_ref[:, cols], 0, 0).astype(BF16)


def combine_kernel(backward, per_head, dec_ref, spread_ref, out_ref):
    count, rows, _ = out_ref.shape
    order = range(count - 1, -1, -1) if backward else range(count)
    for h in range(rows // per_head):
        span = slice(h * per_head, (h + 1) * per_head)
        state = jnp.zeros((per_head, HEAD_DIM), F32)
        for b in order:
            out_ref[b, span] = state.astype(BF16)
            state = dec_ref[b, h] * state + spread_ref[b, span].astype(F32)


def forward_local_kernel(heads, q_ref, k_ref, v_ref, cum_ref, out_ref):
    tokens = q_ref.shape[0]
    size = block_rows(tokens)
    for h in range(heads):
        cols = slice(h * HEAD_DIM, (h + 1) * HEAD_DIM)
        row = cum_ref[h]
        col = column(row)
        for t0 in range(0, tokens, size):
            tr = slice(t0, t0 + size)
            q = q_ref[tr, cols]
            out = None
            for s0 in range(0, t0 + 1, size):
                sr = slice(s0, s0 + size)
                dec = decay_block(col[tr], row[:, sr], s0 == t0)
                p = (mm(q, k_ref[sr, cols], 1, 1) * dec).astype(BF16)
                part = mm(p, v_ref[sr, cols], 1, 0)
                out = part if out is None else out + part
            out_ref[tr, cols] = out


def forward_kernel(heads, near_ref, q_ref, f_ref, gain_ref, cum_ref, state_ref,
                   out_ref, stats_ref, acc_ref):
    step = pl.program_id(0)

    @pl.when(step == 0)
    def _():
        acc_ref[...] = jnp.zeros_like(acc_ref)

    for h in range(heads):
        cols = slice(h * HEAD_DIM, (h + 1) * HEAD_DIM)
        start = column(SCALE * jnp.exp(cum_ref[h]))
        out = near_ref[:, cols] + start * mm(q_ref[:, cols], state_ref[h], 1, 0)
        out_ref[:, cols] = out
        f = f_ref[:, cols].astype(F32)
        go = gain_ref[:, cols] * out
        for i, term in enumerate((out * out, go * go, go * f, f * f)):
            acc_ref[i] += term

    @pl.when(step == pl.num_programs(0) - 1)
    def _():
        for i in range(4):
            stats_ref[i:i + 1, :] = jnp.sum(acc_ref[i].T, axis=0, keepdims=True)


def adjoint_kernel(heads, o_ref, f_ref, q_ref, gain_ref, cum_ref, rows_ref,
                   dout_ref, gsum_ref, back_ref, cols_ref):
    @pl.when(pl.program_id(0) == 0)
    def _():
        for i in range(3):
            cols_ref[i] = column(rows_ref[i:i + 1, :])

    inv_rms, inner, weight = cols_ref[0], cols_ref[1], cols_ref[2]
    for h in range(heads):
        cols = slice(h * HEAD_DIM, (h + 1) * HEAD_DIM)
        gain = gain_ref[:, cols]
        normed = o_ref[:, cols] * inv_rms
        d_err = weight * (gain * normed - f_ref[:, cols].astype(F32))
        d_out = ((d_err * gain - normed * inner) * inv_rms).astype(BF16)
        dout_ref[:, cols] = d_out
        gsum_ref[h] = jnp.sum(d_err * normed, axis=0, keepdims=True)
        start = column(SCALE * jnp.exp(cum_ref[h]))
        qd = (q_ref[:, cols].astype(F32) * start).astype(BF16)
        back_ref[h] = mm(qd, d_out, 0, 0).astype(BF16)


def backward_local_kernel(heads, q_ref, k_ref, v_ref, d_ref, cum_ref, sin_ref,
                          dq_ref, dk_ref, dv_ref):
    tokens = q_ref.shape[0]
    size = block_rows(tokens)
    starts = range(0, tokens, size)
    for h in range(heads):
        cols = slice(h * HEAD_DIM, (h + 1) * HEAD_DIM)
        row = cum_ref[h]
        col = column(row)
        dk, dv = {}, {}
        for t0 in starts:
            tr = slice(t0, t0 + size)
            q = q_ref[tr, cols]
            d = d_ref[tr, cols]
            dq = mm(d, sin_ref[h], 1, 1) * (SCALE * jnp.exp(col[tr]))
            for s0 in range(0, t0 + 1, size):
                sr = slice(s0, s0 + size)
                k = k_ref[sr, cols]
                dec = decay_block(col[tr], row[:, sr], s0 == t0)
                p = (mm(q, k, 1, 1) * dec).astype(BF16)
                g = (mm(d, v_ref[sr, cols], 1, 1) * dec).astype(BF16)
                dq = dq + mm(g, k, 1, 0)
                gq, pd = mm(g, q, 0, 0), mm(p, d, 0, 0)
                dk[s0] = dk[s0] + gq if s0 in dk else gq
                dv[s0] = dv[s0] + pd if s0 in dv else pd
            dq_ref[tr, cols] = dq.astype(BF16)
        for s0 in starts:
            sr = slice(s0, s0 + size)
            dk_ref[sr, cols] = dk[s0]
            dv_ref[sr, cols] = dv[s0]


def backward_kernel(heads, k_ref, v_ref, nk_ref, nv_ref, cum_ref, sout_ref, dk_ref, dv_ref):
    for h in range(heads):
        cols = slice(h * HEAD_DIM, (h + 1) * HEAD_DIM)
        row = cum_ref[h]
        tail = column(jnp.exp(row[:, -1:] - row))
        dk = nk_ref[:, cols] + tail * mm(v_ref[:, cols], sout_ref[h], 1, 1)
        dv = nv_ref[:, cols] + tail * mm(k_ref[:, cols], sout_ref[h], 1, 0)
        dk_ref[:, cols] = dk.astype(BF16)
        dv_ref[:, cols] = dv.astype(BF16)


def split_rows(values):
    high = lax.reduce_precision(values, 8, 7)
    rest = values - high
    middle = lax.reduce_precision(rest, 8, 7)
    parts = jnp.stack([high, middle, rest - middle], axis=1).astype(BF16)
    return jnp.pad(parts, ((0, 0), (0, 13), (0, HEAD_DIM - values.shape[1])))


def join_rows(parts):
    return jnp.sum(parts[:, :3].astype(F32), axis=1)


def local(q, k, v, log_retention, target, gain, weight):
    tokens, width = q.shape
    heads_here = width // HEAD_DIM
    count = lax.axis_size("ctx")
    tokens_all = tokens * count
    heads = 2 if heads_here % 2 == 0 else 1
    grid = (heads_here // heads,)
    entry = HEAD_DIM * HEAD_DIM
    columns = heads_here * entry // count
    rows = columns // HEAD_DIM
    per_head = min(rows, HEAD_DIM)
    owned = rows // per_head

    wide = pl.BlockSpec((tokens, heads * HEAD_DIM), lambda i: (0, i))
    flat = pl.BlockSpec((1, heads * HEAD_DIM), lambda i: (0, i))
    per = pl.BlockSpec((heads, 1, tokens), lambda i: (i, 0, 0))
    mat = pl.BlockSpec((heads, HEAD_DIM, HEAD_DIM), lambda i: (i, 0, 0))
    vec = pl.BlockSpec((heads, 1, HEAD_DIM), lambda i: (i, 0, 0))
    stat = pl.BlockSpec((8, tokens), lambda i: (0, 0))
    mat_shape = jax.ShapeDtypeStruct((heads_here, HEAD_DIM, HEAD_DIM), BF16)
    big = functools.partial(jax.ShapeDtypeStruct, (tokens, width))
    seq = pltpu.CompilerParams(dimension_semantics=("arbitrary",), vmem_limit_bytes=60 << 20)

    cum2 = jnp.cumsum(log_retention, axis=1)
    totals = cum2[:, -1]
    cum = cum2.reshape(heads_here, 1, tokens)
    gain_row = gain.reshape(1, width)

    summary = pl.pallas_call(
        functools.partial(summary_kernel, heads),
        grid=grid, in_specs=[wide, wide, per], out_specs=mat, out_shape=mat_shape,
        compiler_params=seq, name="summary",
    )(k, v, cum)

    def exchange(matrices, extra, read, backward):
        outgoing = jnp.concatenate([matrices.reshape(count, rows, HEAD_DIM), extra], axis=1)
        spread = lax.all_to_all(outgoing, "ctx", split_axis=0, concat_axis=0, tiled=True)
        decay, carry = read(join_rows(spread[:, rows:]))
        combined = pl.pallas_call(
            functools.partial(combine_kernel, backward, per_head),
            in_specs=[pl.BlockSpec(memory_space=pltpu.SMEM),
                      pl.BlockSpec(memory_space=pltpu.VMEM)],
            out_specs=pl.BlockSpec(memory_space=pltpu.VMEM),
            out_shape=jax.ShapeDtypeStruct((count, rows, HEAD_DIM), BF16),
            name="combine",
        )(decay, spread)
        if carry is not None:
            combined = jnp.concatenate([combined, carry], axis=1)
        back = lax.all_to_all(combined, "ctx", split_axis=0, concat_axis=0, tiled=True)
        return back[:, :rows].reshape(heads_here, HEAD_DIM, HEAD_DIM), back[:, rows:], decay

    def everywhere(block):
        return jnp.broadcast_to(block, (count,) + block.shape[1:])

    def read_totals(every):
        first = (lax.axis_index("ctx") * columns) // entry
        return jnp.exp(lax.dynamic_slice(every, (0, first), (count, owned))), None

    square = heads_here * tokens * tokens * HEAD_DIM
    near = pl.pallas_call(
        functools.partial(forward_local_kernel, heads),
        grid=grid, in_specs=[wide, wide, wide, per], out_specs=wide, out_shape=big(F32),
        cost_estimate=pl.CostEstimate(flops=8 * square, bytes_accessed=10 * tokens * width,
                                      transcendentals=square // HEAD_DIM),
        compiler_params=seq, name="forward_local",
    )(q, k, v, cum)

    state_in, _, decay = exchange(
        summary, everywhere(split_rows(totals.reshape(1, heads_here))), read_totals, False)

    attn, stats = pl.pallas_call(
        functools.partial(forward_kernel, heads),
        grid=grid, in_specs=[wide, wide, wide, flat, per, mat],
        out_specs=(wide, pl.BlockSpec((4, tokens), lambda i: (0, 0))),
        out_shape=(big(F32), jax.ShapeDtypeStruct((4, tokens), F32)),
        scratch_shapes=[pltpu.VMEM((4, tokens, HEAD_DIM), F32)],
        compiler_params=seq, name="forward",
    )(near, q, target, gain_row, cum, state_in)

    oo, gg, gf, ff = lax.psum(stats, "head")
    inv_rms = 1.0 / jnp.sqrt(oo / HIDDEN_DIMENSION + EPS)
    pred = gg * inv_rms * inv_rms
    cross = gf * inv_rms
    payoff = (pred - 2.0 * cross + ff) / HIDDEN_DIMENSION
    inner = weight * (pred - cross) / HIDDEN_DIMENSION
    zero = jnp.zeros_like(inner)
    vectors = jnp.stack([inv_rms, inner, weight] + [zero] * 5)

    d_out, gain_sum, back = pl.pallas_call(
        functools.partial(adjoint_kernel, heads),
        grid=grid, in_specs=[wide, wide, wide, flat, per, stat],
        out_specs=(wide, vec, mat),
        out_shape=(big(BF16), jax.ShapeDtypeStruct((heads_here, 1, HEAD_DIM), F32), mat_shape),
        scratch_shapes=[pltpu.VMEM((3, tokens, HEAD_DIM), F32)],
        compiler_params=seq, name="adjoint",
    )(attn, target, q, gain_row, cum, vectors)

    near_q, near_k, near_v = pl.pallas_call(
        functools.partial(backward_local_kernel, heads),
        grid=grid, in_specs=[wide, wide, wide, wide, per, mat],
        out_specs=(wide, wide, wide), out_shape=(big(BF16), big(F32), big(F32)),
        cost_estimate=pl.CostEstimate(flops=20 * square, bytes_accessed=20 * tokens * width,
                                      transcendentals=square // HEAD_DIM),
        compiler_params=seq, name="backward_local",
    )(q, k, v, d_out, cum, state_in)

    def read_gain(every):
        mean = jnp.sum(every, axis=0, keepdims=True) / tokens_all
        return decay, everywhere(split_rows(mean))

    piece = width // count
    state_out, means, _ = exchange(
        back, split_rows(gain_sum.reshape(count, piece)), read_gain, True)
    gain_mean = join_rows(means)[:, :piece].reshape(width)

    dk, dv = pl.pallas_call(
        functools.partial(backward_kernel, heads),
        grid=grid, in_specs=[wide, wide, wide, wide, per, mat],
        out_specs=(wide, wide), out_shape=(big(BF16), big(BF16)),
        compiler_params=seq, name="backward",
    )(k, v, near_k, near_v, cum, state_out)
    return payoff, near_q, dk, dv, gain_mean


def solution(mesh):
    wide = P("ctx", "head")
    return jax.shard_map(
        local,
        mesh=mesh,
        in_specs=(wide, wide, wide, P("head", "ctx"), wide, P("head"), P("ctx")),
        out_specs=(P("ctx"), wide, wide, wide, P("head")),
        check_vma=False,
    )
```
